256 devices in a mesh: head: 8 (over z_hi, core), outer: 2 (over z_lo), inner: 16 (over y, x).
Axes of the slice: x: 4, y: 4, z: 8 (z_hi: 4, z_lo: 2; z = z_hi * 2 + z_lo), core: 2. Of those that a mesh axis runs over, the one named last changes fastest.
Arguments:
- query: bfloat16 [32768, 8192], P(('outer', 'inner', 'head')), may hold values from -100 to 100
- keys: bfloat16 [32768, 1024], P(('outer', 'inner', 'head')), may hold values from -4.5 to 4.5
- values: bfloat16 [32768, 1024], P(('outer', 'inner', 'head')), may hold values from -6 to 6
- lengths: int32 [32], replicated, may hold values from 1 to 2048, 32768 in all
Outputs:
- attended: bfloat16 [32768, 8192], P(('outer', 'inner', 'head'))
The draws below stay inside these ranges and needn't reach their ends.
Inputs may be any that keep to these rules, and one draw needn't show every extreme that they name: `lengths`: they sum to 32768, and the longest is exactly 2048.
All inputs are finite; a program needn't handle non-finite values.
Results may differ from the reference program's by a relative error of at most 0.0038.
Values may be sent and summed in bfloat16 or wider, within the bound.
No kernel may reach another device: no remote copies, remote signals or barrier semaphores. Data moves between devices by JAX's collectives and lax.ppermute only.
A program may use at most 64 MiB of HBM per device.

```python
import math
import jax
import jax.numpy as jnp
import numpy as np
from jax import lax

QUERY_HEAD_COUNT = 64
KEY_VALUE_HEADS = 8
HEAD_SIZE = 128
NEARBY_TOKENS = 1024
PACKED_TOKENS = 32768
REACH = 2
MAXDOC = 2048
NDOCS = 32


def starting_keys(key):
    sampled = jnp.clip(jax.random.normal(jax.random.fold_in(key, 30), (PACKED_TOKENS, KEY_VALUE_HEADS * HEAD_SIZE), jnp.float32), -4.5, 4.5)
    return sampled


def draw_keys(key, part):
    return starting_keys(key).astype(jnp.bfloat16)


def draw_query(key, part):
    result = jnp.clip(jax.random.normal(jax.random.fold_in(key, 40), (PACKED_TOKENS, QUERY_HEAD_COUNT * HEAD_SIZE), jnp.float32), -4.5, 4.5)
    return result.astype(jnp.bfloat16)


def block_levels(key, shape, shards, low, high):
    factor_of = 1.0
    for axis_at, parts in shards:
        steps = jax.random.uniform(jax.random.fold_in(jax.random.fold_in(key, 6), axis_at), (parts,), jnp.float32, low / len(shards), high / len(shards))
        factor_of = factor_of * jnp.repeat(jnp.exp(steps), shape[axis_at] // parts).reshape((-1,) + (1,) * (len(shape) - 1 - axis_at))
    return factor_of


def split_up(amount, total, limit, skew):
    loads = [(1 << 20) // math.isqrt(rank ** skew) + 1 for rank in range(2, amount + 1)]
    rest, given = total - limit - (amount - 1), [1] * (amount - 1)
    while rest > 0:
        candidates = [i for i in range(amount - 1) if given[i] < limit]
        pool, remaining = sum([loads[i] for i in candidates]), rest
        for i in candidates:
            addition = min(limit - given[i], max(1, remaining * loads[i] // pool), rest)
            given[i] = given[i] + addition
            rest = rest - addition
    return np.array([limit] + given)


def uneven_parts(stream_key, amount, total, most, lean):
    if amount == 2:
        one = jax.random.randint(stream_key, (), max(1, total - most), min(most, total - 1) + 1)
        return jnp.stack([one, total - one])
    sizes = jnp.asarray(split_up(amount, total, most, lean), jnp.int32)
    twos = (amount - 1) // 2
    donor, taker = sizes[1:1 + 2 * twos:2], sizes[2:2 + 2 * twos:2]
    margin = jnp.minimum(donor - 1, most - taker)
    shifted = jax.random.randint(jax.random.fold_in(stream_key, 1), (twos,), 0, 1 << 20) % (margin + 1)
    sizes = sizes.at[1:1 + 2 * twos:2].set(donor - shifted).at[2:2 + 2 * twos:2].set(taker + shifted)
    return sizes[jax.random.permutation(jax.random.fold_in(stream_key, 2), amount)]


def scatter_about(own_key, extent, deviation, reach, pieces=(), kind=jnp.bfloat16):
    level = block_levels(own_key, extent, pieces, -0.22, 0.18) if pieces else 1.0
    drawn = jax.random.normal(own_key, extent, jnp.float32) * deviation * level
    return jnp.minimum(jnp.maximum(drawn, -reach), reach).astype(kind)


def setup_inputs(seed: int = 0) -> dict:
    streams_of = jax.random.split(jax.random.key(seed), 5)
    query = draw_query(jax.random.fold_in(streams_of[4], 71), 0)
    keys = draw_keys(jax.random.fold_in(streams_of[4], 71), 0)
    values = scatter_about(streams_of[2], (PACKED_TOKENS, KEY_VALUE_HEADS * HEAD_SIZE), 1.0, 6.0, ((0, 256),))
    lengths = uneven_parts(streams_of[3], NDOCS, PACKED_TOKENS, MAXDOC, 2).astype(jnp.int32)
    return dict(query=query, keys=keys, values=values, lengths=lengths)


def doc_of(lengths, positions):
    ends = jnp.cumsum(lengths)
    return lax.optimization_barrier(jnp.sum((positions[:, None] >= ends[None, :]).astype(jnp.int32), axis=1))

def reference(query, keys, values, lengths):
    group_width = QUERY_HEAD_COUNT // KEY_VALUE_HEADS
    trailing_length = REACH * NEARBY_TOKENS
    key_length = trailing_length + NEARBY_TOKENS
    score_scale = 1.0 / math.sqrt(HEAD_SIZE)
    positions = lax.iota(jnp.int32, PACKED_TOKENS)
    docs = doc_of(lengths, positions)
    filled_keys = jnp.concatenate([jnp.zeros((trailing_length, KEY_VALUE_HEADS * HEAD_SIZE), jnp.bfloat16), keys], 0)
    filled_values = jnp.concatenate([jnp.zeros((trailing_length, KEY_VALUE_HEADS * HEAD_SIZE), jnp.bfloat16), values], 0)
    padded_docs = jnp.concatenate([jnp.full((trailing_length,), -1, jnp.int32), docs], 0)

    def one_block(block_index):
        start_row = (block_index * NEARBY_TOKENS).astype(jnp.int32)
        query_matrix = lax.dynamic_slice_in_dim(query, start_row, NEARBY_TOKENS, 0).astype(jnp.float32)
        query_matrix = query_matrix.reshape(NEARBY_TOKENS, KEY_VALUE_HEADS, group_width, HEAD_SIZE)
        key_matrix = lax.dynamic_slice_in_dim(filled_keys, start_row, key_length, 0).astype(jnp.float32)
        key_matrix = key_matrix.reshape(key_length, KEY_VALUE_HEADS, HEAD_SIZE)
        value_matrix = lax.dynamic_slice_in_dim(filled_values, start_row, key_length, 0).astype(jnp.float32)
        value_matrix = value_matrix.reshape(key_length, KEY_VALUE_HEADS, HEAD_SIZE)
        query_docs = lax.dynamic_slice_in_dim(docs, start_row, NEARBY_TOKENS, 0)
        key_docs = lax.dynamic_slice_in_dim(padded_docs, start_row, key_length, 0)
        query_pos = start_row + lax.iota(jnp.int32, NEARBY_TOKENS)
        key_pos = start_row - trailing_length + lax.iota(jnp.int32, key_length)
        visible = (query_docs[:, None] == key_docs[None, :]) & (key_pos[None, :] <= query_pos[:, None])

        def one_head(operands):
            query_heads, key_heads, value_heads = operands
            scores = jnp.einsum('qgd,cd->gqc', query_heads, key_heads) * score_scale
            masked = jnp.where(visible[None], scores, -1e+30)
            top = lax.optimization_barrier(jnp.max(masked, axis=2))
            weights = jnp.where(visible[None], jnp.exp(masked - top[..., None]), 0.0)
            total = lax.optimization_barrier(jnp.sum(weights, axis=2))
            rounded = lax.optimization_barrier(weights.astype(jnp.bfloat16)).astype(jnp.float32)
            summed = jnp.einsum('gqc,cd->qgd', rounded, value_heads)
            return summed / jnp.transpose(total, (1, 0))[..., None]
        per_head = lax.map(one_head, (jnp.transpose(query_matrix, (1, 0, 2, 3)), jnp.transpose(key_matrix, (1, 0, 2)), jnp.transpose(value_matrix, (1, 0, 2))))
        return jnp.transpose(per_head, (1, 0, 2, 3)).reshape(NEARBY_TOKENS, QUERY_HEAD_COUNT * HEAD_SIZE).astype(jnp.bfloat16)
    blocks = lax.map(one_block, lax.iota(jnp.int32, PACKED_TOKENS // NEARBY_TOKENS))
    return blocks.reshape(PACKED_TOKENS, QUERY_HEAD_COUNT * HEAD_SIZE)
```

```python
import functools
import math

import jax
import jax.numpy as jnp
from jax import lax
from jax.experimental import pallas as pl
from jax.experimental.pallas import tpu as pltpu
from jax.sharding import PartitionSpec as P

HD = 128
GW = 8
KVH = 4
TOK = 128
CHIP = 256
ROWS = GW * TOK
RC = 256
SCALE = math.log2(math.e) / math.sqrt(HD)
NEG = -1e30
MESH_AXES = ("head", "outer", "inner")


def attn_kernel(dists, first, last, *refs):
    nk = len(dists)
    sc, q, st = refs[0], refs[1:3], refs[3]
    ks, vs = refs[4 : 4 + 2 * nk : 2], refs[5 : 5 + 2 * nk : 2]
    pos = 4 + 2 * nk
    if not first:
        m_in, l_in, a_in = refs[pos : pos + 3]
        pos += 3
    if last:
        outs = refs[pos : pos + 2]
        pos += 2
    else:
        m_out, l_out, a_out = refs[pos : pos + 3]
        pos += 3
    qs, bias = refs[pos : pos + 2]
    base = sc[1]

    def run(s, masked):
        for h in range(GW):
            qs[h * TOK : (h + 1) * TOK, :] = q[s][:, h * HD : (h + 1) * HD]
        ones = jnp.ones((CHIP, HD), jnp.bfloat16)
        for r0 in range(0, ROWS, RC):
            scores = []
            for j in range(nk):
                x = lax.dot_general(
                    qs[r0 : r0 + RC, :], ks[j][...], (((1,), (1,)), ((), ())),
                    preferred_element_type=jnp.float32,
                )
                if masked:
                    b = bias[s, :, j * CHIP : (j + 1) * CHIP]
                    x = (x.reshape(RC // TOK, TOK, CHIP) + b[None]).reshape(RC, CHIP)
                scores.append(x)
            top = jnp.max(functools.reduce(jnp.maximum, scores), axis=1, keepdims=True)
            rows = pl.ds(s * ROWS + r0, RC)
            if first:
                shift = top * SCALE
            else:
                before = m_in[0, rows, :]
                top = jnp.maximum(before, top)
                shrink = jnp.exp2((before - top) * SCALE)
                shift = top[:, :1] * SCALE
            both = None
            for j in range(nk):
                p = jnp.exp2(scores[j] * SCALE - shift).astype(jnp.bfloat16)
                d = lax.dot_general(
                    p, jnp.concatenate([vs[j][...], ones], axis=1), (((1,), (0,)), ((), ())),
                    preferred_element_type=jnp.float32,
                )
                both = d if both is None else both + d
            a, l = both[:, :HD], both[:, HD:]
            if not first:
                a = a + a_in[0, rows, :] * shrink
                l = l + l_in[0, rows, :] * shrink
            if last:
                o = (a / l).astype(jnp.bfloat16)
                for i in range(RC // TOK):
                    h = r0 // TOK + i
                    outs[s][:, h * HD : (h + 1) * HD] = o[i * TOK : (i + 1) * TOK, :]
            else:
                m_out[0, rows, :] = jnp.broadcast_to(top, (RC, HD))
                l_out[0, rows, :] = l
                a_out[0, rows, :] = a

    def skip(s):
        if last:
            for h in range(GW):
                rows = pl.ds(s * ROWS + h * TOK, TOK)
                outs[s][:, h * HD : (h + 1) * HD] = (a_in[0, rows, :] / l_in[0, rows, :]).astype(
                    jnp.bfloat16
                )
        else:
            rows = pl.ds(s * ROWS, ROWS)
            m_out[0, rows, :] = m_in[0, rows, :]
            l_out[0, rows, :] = l_in[0, rows, :]
            a_out[0, rows, :] = a_in[0, rows, :]

    for s in range(2):

        @pl.when(pl.program_id(0) == 0)
        def _():
            starts = st[s * TOK : (s + 1) * TOK, :1]
            query_pos = base + sc[6 + s] + lax.broadcasted_iota(jnp.int32, (TOK, CHIP), 0)
            for j, d in enumerate(dists):
                key_pos = base - CHIP * d + lax.broadcasted_iota(jnp.int32, (TOK, CHIP), 1)
                visible = key_pos >= starts
                if d == 0:
                    visible = visible & (key_pos <= query_pos)
                bias[s, :, j * CHIP : (j + 1) * CHIP] = jnp.where(visible, 0.0, NEG)

        if first:
            run(s, True)
        else:
            full = functools.reduce(
                jnp.logical_and, [base - CHIP * d >= sc[3 + 2 * s] for d in dists]
            )
            some = functools.reduce(
                jnp.logical_or, [base - CHIP * d + CHIP > sc[2 + 2 * s] for d in dists]
            )
            pl.when(full)(functools.partial(run, s, False))
            pl.when(some & jnp.logical_not(full))(functools.partial(run, s, True))
            pl.when(jnp.logical_not(some))(functools.partial(skip, s))


def attend(sc, query, query_sibling, starts, pairs, dists, state=None, last=False):
    nk, first = len(dists), state is None
    in_specs = [
        pl.BlockSpec((TOK, GW * HD), lambda g, sc: (0, sc[0] * KVH + g)),
        pl.BlockSpec((TOK, GW * HD), lambda g, sc: (0, g)),
        pl.BlockSpec((CHIP, HD), lambda g, sc: (0, 0)),
    ]
    args = [query, query_sibling, starts]
    for pair in pairs:
        in_specs += [
            pl.BlockSpec((CHIP, HD), lambda g, sc: (0, g)),
            pl.BlockSpec((CHIP, HD), lambda g, sc: (0, KVH + g)),
        ]
        args += [pair, pair]
    state_spec = pl.BlockSpec((1, 2 * ROWS, HD), lambda g, sc: (g, 0, 0))
    if not first:
        in_specs += [state_spec] * 3
        args += list(state)
    if last:
        out_shape = [jax.ShapeDtypeStruct((TOK, KVH * GW * HD), jnp.bfloat16)] * 2
        out_specs = [pl.BlockSpec((TOK, GW * HD), lambda g, sc: (0, g))] * 2
    else:
        out_shape = [jax.ShapeDtypeStruct((KVH, 2 * ROWS, HD), jnp.float32)] * 3
        out_specs = [state_spec] * 3
    return pl.pallas_call(
        functools.partial(attn_kernel, tuple(dists), first, last),
        grid_spec=pltpu.PrefetchScalarGridSpec(
            num_scalar_prefetch=1,
            grid=(KVH,),
            in_specs=in_specs,
            out_specs=out_specs,
            scratch_shapes=[
                pltpu.VMEM((ROWS, HD), jnp.bfloat16),
                pltpu.VMEM((2, TOK, nk * CHIP), jnp.float32),
            ],
        ),
        out_shape=out_shape,
        compiler_params=pltpu.CompilerParams(
            dimension_semantics=("arbitrary",), vmem_limit_bytes=32 << 20
        ),
        cost_estimate=pl.CostEstimate(
            flops=KVH * 2 * ROWS * CHIP * nk * HD * 4, bytes_accessed=24 << 20, transcendentals=0
        ),
        name="attend_" + "_".join(str(d) for d in dists),
    )(sc, *args)


def solution(mesh):
    outer, inner, head = (mesh.shape[axis] for axis in ("outer", "inner", "head"))
    devices = outer * inner * head

    def index_of(block):
        return (block % head) * (outer * inner) + block // head

    def behind(value, chips):
        moves = [(index_of(b), index_of((b + 2 * chips) % devices)) for b in range(devices)]
        return lax.ppermute(value, MESH_AXES, moves)

    def swap(value):
        return lax.ppermute(
            value, MESH_AXES, [(index_of(b), index_of(b ^ 1)) for b in range(devices)]
        )

    def per_device(query, keys, values, lengths):
        block = lax.axis_index(("outer", "inner")) * head + lax.axis_index("head")
        core = lax.rem(block, 2)
        base = (block - core) * TOK
        low = core == 0
        half = KVH * HD

        def halves(first_core, second_core):
            return jnp.concatenate([first_core, second_core], axis=1)

        kv_low = halves(keys[:, :half], values[:, :half])
        kv_high = halves(keys[:, half:], values[:, half:])
        kv_mine = jnp.where(low, kv_low, kv_high)
        kv_sibling = swap(jnp.where(low, kv_high, kv_low))
        r0 = jnp.where(
            low,
            jnp.concatenate([kv_mine, kv_sibling], axis=0),
            jnp.concatenate([kv_sibling, kv_mine], axis=0),
        )
        width = KVH * GW * HD
        query_sibling = swap(jnp.where(low, query[:, width:], query[:, :width]))

        order = lax.iota(jnp.int32, lengths.shape[0])
        ends = jnp.sum(jnp.where(order[None, :] <= order[:, None], lengths[None, :], 0), axis=1)

        def start_of(pos):
            return jnp.max(jnp.where(ends[None, :] <= pos[:, None], ends[None, :], 0), axis=1)

        row = lax.iota(jnp.int32, CHIP)
        offset = lax.rem(row + core * TOK, CHIP)
        starts = jnp.broadcast_to(start_of(base + offset)[:, None], (CHIP, HD))
        i8 = lax.iota(jnp.int32, 8)
        pick = jnp.where(i8 == 3, TOK - 1, jnp.where(i8 == 4, TOK, jnp.where(i8 == 5, CHIP - 1, 0)))
        start8 = start_of(base + lax.rem(pick + core * TOK, CHIP))
        sc = jnp.where(
            i8 == 0, core,
            jnp.where(
                i8 == 1, base,
                jnp.where(i8 == 6, core * TOK, jnp.where(i8 == 7, (1 - core) * TOK, start8)),
            ),
        )

        mid = CHIP // 2
        r1, r4, r8 = behind(r0, 1), behind(r0, 4), behind(r0, 8)
        r3 = behind(r4, -1)
        r5 = behind(r1, 4)
        r2a, r2b = behind(r1[:mid], 1), behind(r3[mid:], -1)
        r7 = behind(r3, 4)
        r2 = jnp.concatenate([r2a, r2b], axis=0)
        r6 = behind(r2, 4)

        call = functools.partial(attend, sc, query, query_sibling, starts)
        state = call([r0, r4, r1], (0, 4, 1))
        state = call([r3, r5, r8], (3, 5, 8), state)
        mine, sibling = call([r2, r7, r6], (2, 7, 6), state, True)
        other = swap(sibling)
        return jnp.where(low, halves(mine, other), halves(other, mine))

    tokens = P(("outer", "inner", "head"), None)
    return jax.shard_map(
        per_device,
        mesh=mesh,
        in_specs=(tokens, tokens, tokens, P()),
        out_specs=tokens,
        check_vma=False,
    )
```

```python
import functools
import math

import jax
import jax.numpy as jnp
from jax import lax
from jax.experimental import pallas as pl
from jax.experimental.pallas import tpu as pltpu
from jax.sharding import PartitionSpec as P

HD = 128
GW = 8
KVH = 4
TOK = 128
CHIP = 256
ROWS = GW * TOK
RC = 256
SCALE = math.log2(math.e) / math.sqrt(HD)
NEG = -1e30
MESH_AXES = ("head", "outer", "inner")
VMEM = pltpu.VMEM


def attn_kernel(dists, first, last, *refs):
    nk = len(dists)
    sc, query, query_sibling, st = refs[:4]
    pairs = refs[4 : 4 + nk]
    pos = 4 + nk
    if not first:
        m_in, l_in, a_in = refs[pos : pos + 3]
        pos += 3
    if last:
        outs = refs[pos : pos + 2]
        pos += 2
    else:
        m_out, l_out, a_out = refs[pos : pos + 3]
        pos += 3
    bias, qs = refs[pos : pos + 2]
    base = sc[1]

    def lanes(start, offset=0):
        return pl.ds(pl.multiple_of(start, HD) + offset, HD)

    def run(s, masked):
        @pl.loop(0, KVH)
        def _(g):
            source = (query, query_sibling)[s]
            shift = sc[0] * (KVH * GW * HD) if s == 0 else 0
            for h in range(GW):
                qs[h * TOK : (h + 1) * TOK, :] = source[:, lanes(shift + g * (GW * HD) + h * HD)]
            ones = jnp.ones((CHIP, HD), jnp.bfloat16)
            ks = [p[:, lanes(g * HD)] for p in pairs]
            vs = [jnp.concatenate([p[:, lanes((KVH + g) * HD)], ones], axis=1) for p in pairs]
            for r0 in range(0, ROWS, RC):
                scores = []
                for j in range(nk):
                    x = lax.dot_general(
                        qs[r0 : r0 + RC, :], ks[j], (((1,), (1,)), ((), ())),
                        preferred_element_type=jnp.float32,
                    )
                    if masked:
                        b = bias[s, :, j * CHIP : (j + 1) * CHIP]
                        x = (x.reshape(RC // TOK, TOK, CHIP) + b[None]).reshape(RC, CHIP)
                    scores.append(x)
                top = jnp.max(functools.reduce(jnp.maximum, scores), axis=1, keepdims=True)
                top = jnp.broadcast_to(top * SCALE, (RC, HD))
                rows = pl.ds(pl.multiple_of((g * 2 + s) * ROWS, ROWS) + r0, RC)
                if not first:
                    before = m_in[rows, :]
                    top = jnp.maximum(before, top)
                    shrink = jnp.exp2(before - top)
                tops = jnp.concatenate([top, top], axis=1)
                both = None
                for j in range(nk):
                    p = jnp.exp2(scores[j] * SCALE - tops).astype(jnp.bfloat16)
                    d = lax.dot_general(
                        p, vs[j], (((1,), (0,)), ((), ())), preferred_element_type=jnp.float32
                    )
                    both = d if both is None else both + d
                a, l = both[:, :HD], both[:, HD:]
                if not first:
                    a = a + a_in[rows, :] * shrink
                    l = l + l_in[rows, :] * shrink
                if last:
                    o = (a / l).astype(jnp.bfloat16)
                    for i in range(RC // TOK):
                        outs[s][:, lanes(g * (GW * HD), r0 // TOK * HD + i * HD)] = o[
                            i * TOK : (i + 1) * TOK, :
                        ]
                else:
                    m_out[rows, :] = top
                    l_out[rows, :] = l
                    a_out[rows, :] = a

    def finish(s):
        @pl.loop(0, KVH)
        def _(g):
            for h in range(GW):
                rows = pl.ds(pl.multiple_of((g * 2 + s) * ROWS, ROWS) + h * TOK, TOK)
                outs[s][:, lanes(g * (GW * HD), h * HD)] = (a_in[rows, :] / l_in[rows, :]).astype(
                    jnp.bfloat16
                )

    for s in range(2):
        starts = st[s * TOK : (s + 1) * TOK, :1]
        query_pos = base + sc[6 + s] + lax.broadcasted_iota(jnp.int32, (TOK, CHIP), 0)
        for j, d in enumerate(dists):
            key_pos = base - CHIP * d + lax.broadcasted_iota(jnp.int32, (TOK, CHIP), 1)
            visible = key_pos >= starts
            if d == 0:
                visible = visible & (key_pos <= query_pos)
            bias[s, :, j * CHIP : (j + 1) * CHIP] = jnp.where(visible, 0.0, NEG)
        if first:
            run(s, True)
        else:
            full = functools.reduce(
                jnp.logical_and, [base - CHIP * d >= sc[3 + 2 * s] for d in dists]
            )
            some = functools.reduce(
                jnp.logical_or, [base - CHIP * d + CHIP > sc[2 + 2 * s] for d in dists]
            )
            pl.when(full)(functools.partial(run, s, False))
            pl.when(some & jnp.logical_not(full))(functools.partial(run, s, True))
            if last:
                pl.when(jnp.logical_not(some))(functools.partial(finish, s))


def attend(sc, query, query_sibling, starts, pairs, dists, state=None, last=False):
    nk, first = len(dists), state is None
    whole = pl.BlockSpec(memory_space=VMEM)
    in_specs = [pl.BlockSpec(memory_space=pltpu.SMEM)] + [whole] * (3 + nk)
    args = [sc, query, query_sibling, starts, *pairs]
    aliases = {}
    if not first:
        if not last:
            aliases = {len(args) + i: i for i in range(3)}
        in_specs += [whole] * 3
        args += [pltpu.with_memory_space_constraint(x, VMEM) for x in state]
    if last:
        out_shape = [jax.ShapeDtypeStruct((TOK, KVH * GW * HD), jnp.bfloat16)] * 2
    else:
        out_shape = [VMEM((KVH * 2 * ROWS, HD), jnp.float32)] * 3
    return pl.pallas_call(
        functools.partial(attn_kernel, tuple(dists), first, last),
        in_specs=in_specs,
        out_specs=[whole] * len(out_shape),
        out_shape=out_shape,
        scratch_shapes=[VMEM((2, TOK, nk * CHIP), jnp.float32), VMEM((ROWS, HD), jnp.bfloat16)],
        input_output_aliases=aliases,
        compiler_params=pltpu.CompilerParams(vmem_limit_bytes=30 << 20),
        cost_estimate=pl.CostEstimate(
            flops=KVH * 2 * ROWS * CHIP * nk * HD * 4, bytes_accessed=4 << 20, transcendentals=0
        ),
        name="attend_" + "_".join(str(d) for d in dists),
    )(*args)


def solution(mesh):
    outer, inner, head = (mesh.shape[axis] for axis in ("outer", "inner", "head"))
    devices = outer * inner * head

    def index_of(block):
        return (block % head) * (outer * inner) + block // head

    def behind(value, chips):
        moves = [(index_of(b), index_of((b + 2 * chips) % devices)) for b in range(devices)]
        return lax.ppermute(value, MESH_AXES, moves)

    def swap(value):
        return lax.ppermute(
            value, MESH_AXES, [(index_of(b), index_of(b ^ 1)) for b in range(devices)]
        )

    def after(value, state):
        value, top = lax.optimization_barrier((value, state[0]))
        return value, [top, *state[1:]]

    def per_device(query, keys, values, lengths):
        block = lax.axis_index(("outer", "inner")) * head + lax.axis_index("head")
        core = lax.rem(block, 2)
        base = (block - core) * TOK
        low = core == 0
        half = KVH * HD

        def halves(first_core, second_core):
            return jnp.concatenate([first_core, second_core], axis=1)

        kv_low = halves(keys[:, :half], values[:, :half])
        kv_high = halves(keys[:, half:], values[:, half:])
        kv_mine = jnp.where(low, kv_low, kv_high)
        kv_sibling = swap(jnp.where(low, kv_high, kv_low))
        r0 = jnp.where(
            low,
            jnp.concatenate([kv_mine, kv_sibling], axis=0),
            jnp.concatenate([kv_sibling, kv_mine], axis=0),
        )
        width = KVH * GW * HD
        query_sibling = swap(jnp.where(low, query[:, width:], query[:, :width]))

        order = lax.iota(jnp.int32, lengths.shape[0])
        ends = jnp.sum(jnp.where(order[None, :] <= order[:, None], lengths[None, :], 0), axis=1)

        def start_of(pos):
            return jnp.max(jnp.where(ends[None, :] <= pos[:, None], ends[None, :], 0), axis=1)

        row = lax.iota(jnp.int32, CHIP)
        offset = lax.rem(row + core * TOK, CHIP)
        starts = jnp.broadcast_to(start_of(base + offset)[:, None], (CHIP, HD))
        i8 = lax.iota(jnp.int32, 8)
        pick = jnp.where(i8 == 3, TOK - 1, jnp.where(i8 == 4, TOK, jnp.where(i8 == 5, CHIP - 1, 0)))
        start8 = start_of(base + lax.rem(pick + core * TOK, CHIP))
        sc = jnp.where(
            i8 == 0, core,
            jnp.where(
                i8 == 1, base,
                jnp.where(i8 == 6, core * TOK, jnp.where(i8 == 7, (1 - core) * TOK, start8)),
            ),
        )

        call = functools.partial(attend, sc, query, query_sibling, starts)
        r4, r1 = behind(r0, 4), behind(r0, 1)
        r3, r8 = behind(r4, -1), behind(r0, 8)
        state = call([r0, r4], (0, 4))
        r1, state = after(r1, state)
        r2, r5 = behind(r1, 1), behind(r1, 4)
        state = call([r1, r8], (1, 8), state)
        r3, state = after(r3, state)
        r7 = behind(r3, 4)
        state = call([r3, r5], (3, 5), state)
        r2, state = after(r2, state)
        r6 = behind(r2, 4)
        state = call([r2, r7], (2, 7), state)
        mine, sibling = call([r6], (6,), state, True)
        other = swap(sibling)
        return jnp.where(low, halves(mine, other), halves(other, mine))

    tokens = P(("outer", "inner", "head"), None)
    return jax.shard_map(
        per_device,
        mesh=mesh,
        in_specs=(tokens, tokens, tokens, P()),
        out_specs=tokens,
        check_vma=False,
    )
```

```python
import functools
import math

import jax
import jax.numpy as jnp
from jax import lax
from jax.experimental import pallas as pl
from jax.experimental.pallas import tpu as pltpu
from jax.sharding import PartitionSpec as P

HD = 128
GW = 8
KVH = 4
TOK = 128
CHIP = 256
ROWS = GW * TOK
RC = 256
SCALE = math.log2(math.e) / math.sqrt(HD)
NEG = -1e30
MESH_AXES = ("head", "outer", "inner")
VMEM = pltpu.VMEM


def attn_kernel(dists, parts, first, last, sides, *refs):
    nk = len(dists)
    sc, query, query_sibling, st = refs[:4]
    pos = 4
    pairs = []
    for part in parts:
        count = 1 if part == "one" else 2
        pairs.append((part, refs[pos : pos + count]))
        pos += count
    if not first:
        m_in, l_in, a_in = refs[pos : pos + 3]
        pos += 3
    if last:
        outs = dict(zip(sides, refs[pos : pos + len(sides)]))
        pos += len(sides)
    else:
        m_out, l_out, a_out = refs[pos : pos + 3]
        pos += 3
    bias, qs = refs[pos : pos + 2]
    base = sc[1]

    def lanes(start, offset=0):
        return pl.ds(pl.multiple_of(start, HD) + offset, HD)

    def columns(pair, at):
        part, arrays = pair
        loaded = [array[:, at] for array in arrays]
        if part == "cat":
            return jnp.concatenate(loaded, axis=0)
        return loaded[0] + loaded[1] if part == "add" else loaded[0]

    def run(s, masked):
        @pl.loop(0, KVH)
        def _(g):
            source = (query, query_sibling)[s]
            shift = sc[0] * (KVH * GW * HD) if s == 0 else 0
            for h in range(GW):
                qs[h * TOK : (h + 1) * TOK, :] = source[:, lanes(shift + g * (GW * HD) + h * HD)]
            ones = jnp.ones((CHIP, HD), jnp.bfloat16)
            ks = [columns(p, lanes(g * HD)) for p in pairs]
            vs = [
                jnp.concatenate([columns(p, lanes((KVH + g) * HD)), ones], axis=1) for p in pairs
            ]
            for r0 in range(0, ROWS, RC):
                scores = []
                for j in range(nk):
                    x = lax.dot_general(
                        qs[r0 : r0 + RC, :], ks[j], (((1,), (1,)), ((), ())),
                        preferred_element_type=jnp.float32,
                    )
                    if masked:
                        b = bias[s, :, j * CHIP : (j + 1) * CHIP]
                        x = (x.reshape(RC // TOK, TOK, CHIP) + b[None]).reshape(RC, CHIP)
                    scores.append(x)
                top = jnp.max(functools.reduce(jnp.maximum, scores), axis=1, keepdims=True)
                top = jnp.broadcast_to(top * SCALE, (RC, HD))
                rows = pl.ds(pl.multiple_of((g * 2 + s) * ROWS, ROWS) + r0, RC)
                if not first:
                    before = m_in[rows, :]
                    top = jnp.maximum(before, top)
                    shrink = jnp.exp2(before - top)
                tops = jnp.concatenate([top, top], axis=1)
                both = None
                for j in range(nk):
                    p = jnp.exp2(scores[j] * SCALE - tops).astype(jnp.bfloat16)
                    d = lax.dot_general(
                        p, vs[j], (((1,), (0,)), ((), ())), preferred_element_type=jnp.float32
                    )
                    both = d if both is None else both + d
                a, l = both[:, :HD], both[:, HD:]
                if not first:
                    a = a + a_in[rows, :] * shrink
                    l = l + l_in[rows, :] * shrink
                if last:
                    o = (a / l).astype(jnp.bfloat16)
                    for i in range(RC // TOK):
                        outs[s][:, lanes(g * (GW * HD), r0 // TOK * HD + i * HD)] = o[
                            i * TOK : (i + 1) * TOK, :
                        ]
                else:
                    m_out[rows, :] = top
                    l_out[rows, :] = l
                    a_out[rows, :] = a

    def finish(s):
        @pl.loop(0, KVH)
        def _(g):
            for h in range(GW):
                rows = pl.ds(pl.multiple_of((g * 2 + s) * ROWS, ROWS) + h * TOK, TOK)
                outs[s][:, lanes(g * (GW * HD), h * HD)] = (a_in[rows, :] / l_in[rows, :]).astype(
                    jnp.bfloat16
                )

    for s in sides:
        starts = st[s * TOK : (s + 1) * TOK, :1]
        query_pos = base + sc[6 + s] + lax.broadcasted_iota(jnp.int32, (TOK, CHIP), 0)
        for j, d in enumerate(dists):
            key = lax.broadcasted_iota(jnp.int32, (TOK, CHIP), 1)
            key_pos = base - CHIP * d + ((key + sc[6]) & (CHIP - 1))
            visible = key_pos >= starts
            if d == 0:
                visible = visible & (key_pos <= query_pos)
            bias[s, :, j * CHIP : (j + 1) * CHIP] = jnp.where(visible, 0.0, NEG)
        if first:
            run(s, True)
        else:
            full = functools.reduce(
                jnp.logical_and, [base - CHIP * d >= sc[3 + 2 * s] for d in dists]
            )
            some = functools.reduce(
                jnp.logical_or, [base - CHIP * d + CHIP > sc[2 + 2 * s] for d in dists]
            )
            pl.when(full)(functools.partial(run, s, False))
            pl.when(some & jnp.logical_not(full))(functools.partial(run, s, True))
            if last:
                pl.when(jnp.logical_not(some))(functools.partial(finish, s))


def attend(sc, query, query_sibling, starts, pairs, dists, state=None, last=False, sides=(0, 1)):
    nk, first = len(dists), state is None
    whole = pl.BlockSpec(memory_space=VMEM)
    parts = tuple(pair[0] if isinstance(pair, tuple) else "one" for pair in pairs)
    args = [sc, query, query_sibling, starts]
    for pair in pairs:
        args += pair[1:] if isinstance(pair, tuple) else [pair]
    in_specs = [pl.BlockSpec(memory_space=pltpu.SMEM)] + [whole] * (len(args) - 1)
    aliases = {}
    if not first:
        if not last:
            aliases = {len(args) + i: i for i in range(3)}
        in_specs += [whole] * 3
        args += [pltpu.with_memory_space_constraint(x, VMEM) for x in state]
    if last:
        out_shape = [jax.ShapeDtypeStruct((TOK, KVH * GW * HD), jnp.bfloat16)] * len(sides)
    else:
        out_shape = [VMEM((KVH * 2 * ROWS, HD), jnp.float32)] * 3
    return pl.pallas_call(
        functools.partial(attn_kernel, tuple(dists), parts, first, last, sides),
        in_specs=in_specs,
        out_specs=[whole] * len(out_shape),
        out_shape=out_shape,
        scratch_shapes=[VMEM((2, TOK, nk * CHIP), jnp.float32), VMEM((ROWS, HD), jnp.bfloat16)],
        input_output_aliases=aliases,
        compiler_params=pltpu.CompilerParams(vmem_limit_bytes=16 << 20),
        cost_estimate=pl.CostEstimate(
            flops=KVH * len(sides) * ROWS * CHIP * nk * HD * 4, bytes_accessed=4 << 20, transcendentals=0
        ),
        name="attend_" + "_".join(str(d) for d in dists) + ("" if len(sides) == 2 else "ab"[sides[0]]),
    )(*args)


def solution(mesh):
    outer, inner, head = (mesh.shape[axis] for axis in ("outer", "inner", "head"))
    devices = outer * inner * head

    def index_of(block):
        return (block % head) * (outer * inner) + block // head

    chips_all = devices // 2

    def send(value, moves):
        pairs = [(index_of(2 * a + k), index_of(2 * b + k)) for a, b in moves for k in range(2)]
        return lax.ppermute(value, MESH_AXES, pairs)

    def behind(value, chips, wrap=()):
        moves = [(c, (c + chips) % chips_all) for c in range(chips_all)]
        return send(value, [(c, d) for c, d in moves if d == c + chips or d in wrap])

    def swap(value):
        return lax.ppermute(
            value, MESH_AXES, [(index_of(b), index_of(b ^ 1)) for b in range(devices)]
        )

    def after(value, state):
        value, top = lax.optimization_barrier((value, state[0]))
        return value, [top, *state[1:]]

    def per_device(query, keys, values, lengths):
        block = lax.axis_index(("outer", "inner")) * head + lax.axis_index("head")
        core = lax.rem(block, 2)
        base = (block - core) * TOK
        low = core == 0
        half = KVH * HD

        def halves(first_core, second_core):
            return jnp.concatenate([first_core, second_core], axis=1)

        def heads_of(array, which, size):
            return lax.dynamic_slice_in_dim(array, which * size, size, 1)

        kv_mine = halves(heads_of(keys, core, half), heads_of(values, core, half))
        kv_send = halves(heads_of(keys, 1 - core, half), heads_of(values, 1 - core, half))
        width = KVH * GW * HD
        query_send, kv_send = lax.optimization_barrier((query, kv_send))
        query_send = heads_of(query_send, 1 - core, width)
        kv_sibling, query_send = lax.optimization_barrier((swap(kv_send), query_send))
        r0 = jnp.concatenate([kv_mine, kv_sibling], axis=0)
        query_sibling = swap(query_send)

        order = lax.iota(jnp.int32, lengths.shape[0])
        ends = jnp.sum(jnp.where(order[None, :] <= order[:, None], lengths[None, :], 0), axis=1)

        def start_of(pos):
            return jnp.max(jnp.where(ends[None, :] <= pos[:, None], ends[None, :], 0), axis=1)

        row = lax.iota(jnp.int32, CHIP)
        offset = lax.rem(row + core * TOK, CHIP)
        starts = jnp.broadcast_to(start_of(base + offset)[:, None], (CHIP, HD))
        i8 = lax.iota(jnp.int32, 8)
        pick = jnp.where(i8 == 3, TOK - 1, jnp.where(i8 == 4, TOK, jnp.where(i8 == 5, CHIP - 1, 0)))
        start8 = start_of(base + lax.rem(pick + core * TOK, CHIP))
        sc = jnp.where(
            i8 == 0, core,
            jnp.where(
                i8 == 1, base,
                jnp.where(i8 == 6, core * TOK, jnp.where(i8 == 7, (1 - core) * TOK, start8)),
            ),
        )

        call = functools.partial(attend, sc, query, query_sibling, starts)
        mid = CHIP // 2
        r4, r1, r8 = behind(r0, 4, (0, 1)), behind(r0, 1), behind(r0, 8, (0,))
        state = call([r0], (0,))
        r4, state = after(r4, state)
        r3 = behind(r4, -1, (127,))
        r2a, r5 = behind(r1[:mid], 1), behind(r1, 4)
        state = call([r4, r1], (4, 1), state)
        r8, state = after(r8, state)
        r7 = behind(r8, -1, (127,))
        r2b = behind(r3[mid:], -1, (127,))
        r6a = behind(r2a, 4)
        state = call([r3, r8], (3, 8), state)
        r2b, state = after(r2b, state)
        r6b = behind(r2b, 4)
        state = call([("cat", r2a, r2b), r5], (2, 5), state)
        mine, sibling = call([r7, ("cat", r6a, r6b)], (7, 6), state, True)
        other = swap(sibling)
        return jnp.where(low, halves(mine, other), halves(other, mine))

    tokens = P(("outer", "inner", "head"), None)
    return jax.shard_map(
        per_device,
        mesh=mesh,
        in_specs=(tokens, tokens, tokens, P()),
        out_specs=tokens,
        check_vma=False,
    )
```

```python
import functools
import math

import jax
import jax.numpy as jnp
from jax import lax
from jax.experimental import pallas as pl
from jax.experimental.pallas import tpu as pltpu
from jax.sharding import PartitionSpec as P

HD = 128
GW = 8
KVH = 4
TOK = 128
CHIP = 256
ROWS = GW * TOK
RC = 256
SCALE = math.log2(math.e) / math.sqrt(HD)
NEG = -1e30
MESH_AXES = ("head", "outer", "inner")
VMEM = pltpu.VMEM


def attn_kernel(dists, parts, first, last, sides, *refs):
    nk = len(dists)
    sc, query, query_sibling, st = refs[:4]
    pos = 4
    pairs = []
    for part in parts:
        count = 1 if part == "one" else 2
        pairs.append((part, refs[pos : pos + count]))
        pos += count
    if not first:
        m_in, l_in, a_in = refs[pos : pos + 3]
        pos += 3
    if last:
        outs = dict(zip(sides, refs[pos : pos + len(sides)]))
        pos += len(sides)
    else:
        m_out, l_out, a_out = refs[pos : pos + 3]
        pos += 3
    bias, qs = refs[pos : pos + 2]
    base = sc[1]

    def lanes(start, offset=0):
        return pl.ds(pl.multiple_of(start, HD) + offset, HD)

    def columns(pair, at):
        part, arrays = pair
        loaded = [array[:, at] for array in arrays]
        if part == "cat":
            return jnp.concatenate(loaded, axis=0)
        return loaded[0] + loaded[1] if part == "add" else loaded[0]

    def run(s, masked):
        @pl.loop(0, KVH)
        def _(g):
            source = (query, query_sibling)[s]
            shift = sc[0] * (KVH * GW * HD) if s == 0 else 0
            for h in range(GW):
                qs[h * TOK : (h + 1) * TOK, :] = source[:, lanes(shift + g * (GW * HD) + h * HD)]
            ones = jnp.ones((CHIP, HD), jnp.bfloat16)
            ks = [columns(p, lanes(g * HD)) for p in pairs]
            vs = [
                jnp.concatenate([columns(p, lanes((KVH + g) * HD)), ones], axis=1) for p in pairs
            ]
            for r0 in range(0, ROWS, RC):
                scores = []
                for j in range(nk):
                    x = lax.dot_general(
                        qs[r0 : r0 + RC, :], ks[j], (((1,), (1,)), ((), ())),
                        preferred_element_type=jnp.float32,
                    )
                    if masked:
                        b = bias[s, :, j * CHIP : (j + 1) * CHIP]
                        x = (x.reshape(RC // TOK, TOK, CHIP) + b[None]).reshape(RC, CHIP)
                    scores.append(x)
                top = jnp.max(functools.reduce(jnp.maximum, scores), axis=1, keepdims=True)
                top = jnp.broadcast_to(top * SCALE, (RC, HD))
                rows = pl.ds(pl.multiple_of((g * 2 + s) * ROWS, ROWS) + r0, RC)
                if not first:
                    before = m_in[rows, :]
                    top = jnp.maximum(before, top)
                    shrink = jnp.exp2(before - top)
                tops = jnp.concatenate([top, top], axis=1)
                both = None
                for j in range(nk):
                    p = jnp.exp2(scores[j] * SCALE - tops).astype(jnp.bfloat16)
                    d = lax.dot_general(
                        p, vs[j], (((1,), (0,)), ((), ())), preferred_element_type=jnp.float32
                    )
                    both = d if both is None else both + d
                a, l = both[:, :HD], both[:, HD:]
                if not first:
                    a = a + a_in[rows, :] * shrink
                    l = l + l_in[rows, :] * shrink
                if last:
                    o = (a / l).astype(jnp.bfloat16)
                    for i in range(RC // TOK):
                        outs[s][:, lanes(g * (GW * HD), r0 // TOK * HD + i * HD)] = o[
                            i * TOK : (i + 1) * TOK, :
                        ]
                else:
                    m_out[rows, :] = top
                    l_out[rows, :] = l
                    a_out[rows, :] = a

    def finish(s):
        @pl.loop(0, KVH)
        def _(g):
            for h in range(GW):
                rows = pl.ds(pl.multiple_of((g * 2 + s) * ROWS, ROWS) + h * TOK, TOK)
                outs[s][:, lanes(g * (GW * HD), h * HD)] = (a_in[rows, :] / l_in[rows, :]).astype(
                    jnp.bfloat16
                )

    for s in sides:
        starts = st[s * TOK : (s + 1) * TOK, :1]
        query_pos = base + sc[6 + s] + lax.broadcasted_iota(jnp.int32, (TOK, CHIP), 0)
        for j, d in enumerate(dists):
            key = lax.broadcasted_iota(jnp.int32, (TOK, CHIP), 1)
            key_pos = base - CHIP * d + ((key + sc[6]) & (CHIP - 1))
            visible = key_pos >= starts
            if d == 0:
                visible = visible & (key_pos <= query_pos)
            bias[s, :, j * CHIP : (j + 1) * CHIP] = jnp.where(visible, 0.0, NEG)
        if first:
            run(s, True)
        else:
            full = functools.reduce(
                jnp.logical_and, [base - CHIP * d >= sc[3 + 2 * s] for d in dists]
            )
            some = functools.reduce(
                jnp.logical_or, [base - CHIP * d + CHIP > sc[2 + 2 * s] for d in dists]
            )
            pl.when(full)(functools.partial(run, s, False))
            pl.when(some & jnp.logical_not(full))(functools.partial(run, s, True))
            if last:
                pl.when(jnp.logical_not(some))(functools.partial(finish, s))


def attend(sc, query, query_sibling, starts, pairs, dists, state=None, last=False, sides=(0, 1)):
    nk, first = len(dists), state is None
    whole = pl.BlockSpec(memory_space=VMEM)
    parts = tuple(pair[0] if isinstance(pair, tuple) else "one" for pair in pairs)
    args = [sc, query, query_sibling, starts]
    for pair in pairs:
        args += pair[1:] if isinstance(pair, tuple) else [pair]
    in_specs = [pl.BlockSpec(memory_space=pltpu.SMEM)] + [whole] * (len(args) - 1)
    aliases = {}
    if not first:
        if not last:
            aliases = {len(args) + i: i for i in range(3)}
        in_specs += [whole] * 3
        args += [pltpu.with_memory_space_constraint(x, VMEM) for x in state]
    if last:
        out_shape = [VMEM((TOK, KVH * GW * HD), jnp.bfloat16)] * len(sides)
    else:
        out_shape = [VMEM((KVH * 2 * ROWS, HD), jnp.float32)] * 3
    return pl.pallas_call(
        functools.partial(attn_kernel, tuple(dists), parts, first, last, sides),
        in_specs=in_specs,
        out_specs=[whole] * len(out_shape),
        out_shape=out_shape,
        scratch_shapes=[VMEM((2, TOK, nk * CHIP), jnp.float32), VMEM((ROWS, HD), jnp.bfloat16)],
        input_output_aliases=aliases,
        compiler_params=pltpu.CompilerParams(vmem_limit_bytes=16 << 20),
        cost_estimate=pl.CostEstimate(
            flops=KVH * len(sides) * ROWS * CHIP * nk * HD * 4, bytes_accessed=4 << 20, transcendentals=0
        ),
        name="attend_" + "_".join(str(d) for d in dists) + ("" if len(sides) == 2 else "ab"[sides[0]]),
    )(*args)


def join_kernel(sc, mine, other, out, sems):
    width = KVH * GW * HD
    copies = [
        pltpu.make_async_copy(
            part, out.at[:, pl.ds(pl.multiple_of(core * width, width), width)], sems.at[i]
        )
        for i, (part, core) in enumerate(((mine, sc[0]), (other, 1 - sc[0])))
    ]
    for copy in copies:
        copy.start()
    for copy in copies:
        copy.wait()


def join(sc, mine, other):
    whole = pl.BlockSpec(memory_space=VMEM)
    return pl.pallas_call(
        join_kernel,
        in_specs=[pl.BlockSpec(memory_space=pltpu.SMEM), whole, whole],
        out_specs=pl.BlockSpec(memory_space=pl.ANY),
        out_shape=jax.ShapeDtypeStruct((TOK, 2 * KVH * GW * HD), jnp.bfloat16),
        scratch_shapes=[pltpu.SemaphoreType.DMA((2,))],
        compiler_params=pltpu.CompilerParams(vmem_limit_bytes=16 << 20),
        name="join",
    )(sc, pltpu.with_memory_space_constraint(mine, VMEM), other)


def solution(mesh):
    outer, inner, head = (mesh.shape[axis] for axis in ("outer", "inner", "head"))
    devices = outer * inner * head

    def index_of(block):
        return (block % head) * (outer * inner) + block // head

    chips_all = devices // 2

    def send(value, moves):
        pairs = [(index_of(2 * a + k), index_of(2 * b + k)) for a, b in moves for k in range(2)]
        return lax.ppermute(value, MESH_AXES, pairs)

    def behind(value, chips, wrap=()):
        moves = [(c, (c + chips) % chips_all) for c in range(chips_all)]
        return send(value, [(c, d) for c, d in moves if d == c + chips or d in wrap])

    def swap(value):
        return lax.ppermute(
            value, MESH_AXES, [(index_of(b), index_of(b ^ 1)) for b in range(devices)]
        )

    def after(value, state):
        value, top = lax.optimization_barrier((value, state[0]))
        return value, [top, *state[1:]]

    def per_device(query, keys, values, lengths):
        block = lax.axis_index(("outer", "inner")) * head + lax.axis_index("head")
        core = lax.rem(block, 2)
        base = (block - core) * TOK
        half = KVH * HD

        def halves(first_core, second_core):
            return jnp.concatenate([first_core, second_core], axis=1)

        def heads_of(array, which, size):
            return lax.dynamic_slice_in_dim(array, which * size, size, 1)

        kv_mine = halves(heads_of(keys, core, half), heads_of(values, core, half))
        kv_send = halves(heads_of(keys, 1 - core, half), heads_of(values, 1 - core, half))
        width = KVH * GW * HD
        query_send, kv_send = lax.optimization_barrier((query, kv_send))
        query_send = heads_of(query_send, 1 - core, width)
        kv_sibling, query_send = lax.optimization_barrier((swap(kv_send), query_send))
        r0 = jnp.concatenate([kv_mine, kv_sibling], axis=0)
        query_sibling = swap(query_send)

        order = lax.iota(jnp.int32, lengths.shape[0])
        ends = jnp.sum(jnp.where(order[None, :] <= order[:, None], lengths[None, :], 0), axis=1)

        def start_of(pos):
            return jnp.max(jnp.where(ends[None, :] <= pos[:, None], ends[None, :], 0), axis=1)

        row = lax.iota(jnp.int32, CHIP)
        offset = lax.rem(row + core * TOK, CHIP)
        starts = jnp.broadcast_to(start_of(base + offset)[:, None], (CHIP, HD))
        i8 = lax.iota(jnp.int32, 8)
        pick = jnp.where(i8 == 3, TOK - 1, jnp.where(i8 == 4, TOK, jnp.where(i8 == 5, CHIP - 1, 0)))
        start8 = start_of(base + lax.rem(pick + core * TOK, CHIP))
        sc = jnp.where(
            i8 == 0, core,
            jnp.where(
                i8 == 1, base,
                jnp.where(i8 == 6, core * TOK, jnp.where(i8 == 7, (1 - core) * TOK, start8)),
            ),
        )

        call = functools.partial(attend, sc, query, query_sibling, starts)
        mid = CHIP // 2
        r4, r1, r8 = behind(r0, 4, (0, 1)), behind(r0, 1), behind(r0, 8, (0,))
        state = call([r0], (0,))
        r4, state = after(r4, state)
        r3 = behind(r4, -1, (127,))
        r2a, r5 = behind(r1[:mid], 1), behind(r1, 4)
        state = call([r4, r1], (4, 1), state)
        r8, state = after(r8, state)
        r7 = behind(r8, -1, (127,))
        r2b = behind(r3[mid:], -1, (127,))
        r6a = behind(r2a, 4)
        state = call([r3, r8], (3, 8), state)
        r2b, state = after(r2b, state)
        r6b = behind(r2b, 4)
        state = call([("cat", r2a, r2b), r5], (2, 5), state)
        mine, sibling = call([r7, ("cat", r6a, r6b)], (7, 6), state, True)
        return join(sc, mine, swap(sibling))

    tokens = P(("outer", "inner", "head"), None)
    return jax.shard_map(
        per_device,
        mesh=mesh,
        in_specs=(tokens, tokens, tokens, P()),
        out_specs=tokens,
        check_vma=False,
    )
```

```python
import functools
import math

import jax
import jax.numpy as jnp
from jax import lax
from jax.experimental import pallas as pl
from jax.experimental.pallas import tpu as pltpu
from jax.sharding import PartitionSpec as P

HD = 128
GW = 8
KVH = 4
TOK = 128
CHIP = 256
ROWS = GW * TOK
RC = 128
SCALE = math.log2(math.e) / math.sqrt(HD)
NEG = -1e30
MESH_AXES = ("head", "outer", "inner")
VMEM = pltpu.VMEM


def attn_kernel(dists, parts, first, last, sides, *refs):
    nk = len(dists)
    sc, query, query_sibling, st = refs[:4]
    pos = 4
    pairs = []
    for part in parts:
        count = 1 if part == "one" else 2
        pairs.append((part, refs[pos : pos + count]))
        pos += count
    if not first:
        m_in, l_in, a_in = refs[pos : pos + 3]
        pos += 3
    if last:
        outs = dict(zip(sides, refs[pos : pos + len(sides)]))
        pos += len(sides)
    else:
        m_out, l_out, a_out = refs[pos : pos + 3]
        pos += 3
    bias, qs = refs[pos : pos + 2]
    base = sc[1]

    def lanes(start, offset=0):
        return pl.ds(pl.multiple_of(start, HD) + offset, HD)

    def columns(pair, at):
        part, arrays = pair
        loaded = [array[:, at] for array in arrays]
        if part == "cat":
            return jnp.concatenate(loaded, axis=0)
        return loaded[0] + loaded[1] if part == "add" else loaded[0]

    def run(s, masked):
        @pl.loop(0, KVH)
        def _(g):
            source = (query, query_sibling)[s]
            shift = sc[0] * (KVH * GW * HD) if s == 0 else 0
            for h in range(GW):
                qs[h * TOK : (h + 1) * TOK, :] = source[:, lanes(shift + g * (GW * HD) + h * HD)]
            ones = jnp.ones((CHIP, HD), jnp.bfloat16)
            ks = [columns(p, lanes(g * HD)) for p in pairs]
            vs = [
                jnp.concatenate([columns(p, lanes((KVH + g) * HD)), ones], axis=1) for p in pairs
            ]
            for r0 in range(0, ROWS, RC):
                scores = []
                for j in range(nk):
                    x = lax.dot_general(
                        qs[r0 : r0 + RC, :], ks[j], (((1,), (1,)), ((), ())),
                        preferred_element_type=jnp.float32,
                    )
                    if masked:
                        b = bias[s, :, j * CHIP : (j + 1) * CHIP]
                        x = (x.reshape(RC // TOK, TOK, CHIP) + b[None]).reshape(RC, CHIP)
                    scores.append(x)
                top = jnp.max(functools.reduce(jnp.maximum, scores), axis=1, keepdims=True)
                top = jnp.broadcast_to(top * SCALE, (RC, HD))
                rows = pl.ds(pl.multiple_of((g * 2 + s) * ROWS, ROWS) + r0, RC)
                if not first:
                    before = m_in[rows, :]
                    top = jnp.maximum(before, top)
                    shrink = jnp.exp2(before - top)
                tops = jnp.concatenate([top, top], axis=1)
                both = None
                for j in range(nk):
                    p = jnp.exp2(scores[j] * SCALE - tops).astype(jnp.bfloat16)
                    d = lax.dot_general(
                        p, vs[j], (((1,), (0,)), ((), ())), preferred_element_type=jnp.float32
                    )
                    both = d if both is None else both + d
                a, l = both[:, :HD], both[:, HD:]
                if not first:
                    a = a + a_in[rows, :] * shrink
                    l = l + l_in[rows, :] * shrink
                if last:
                    o = (a / l).astype(jnp.bfloat16)
                    for i in range(RC // TOK):
                        outs[s][:, lanes(g * (GW * HD), r0 // TOK * HD + i * HD)] = o[
                            i * TOK : (i + 1) * TOK, :
                        ]
                else:
                    m_out[rows, :] = top
                    l_out[rows, :] = l
                    a_out[rows, :] = a

    def finish(s):
        @pl.loop(0, KVH)
        def _(g):
            for h in range(GW):
                rows = pl.ds(pl.multiple_of((g * 2 + s) * ROWS, ROWS) + h * TOK, TOK)
                outs[s][:, lanes(g * (GW * HD), h * HD)] = (a_in[rows, :] / l_in[rows, :]).astype(
                    jnp.bfloat16
                )

    for s in sides:
        starts = st[s * TOK : (s + 1) * TOK, :1]
        query_pos = base + sc[6 + s] + lax.broadcasted_iota(jnp.int32, (TOK, CHIP), 0)
        for j, d in enumerate(dists):
            key = lax.broadcasted_iota(jnp.int32, (TOK, CHIP), 1)
            key_pos = base - CHIP * d + ((key + sc[6]) & (CHIP - 1))
            visible = key_pos >= starts
            if d == 0:
                visible = visible & (key_pos <= query_pos)
            bias[s, :, j * CHIP : (j + 1) * CHIP] = jnp.where(visible, 0.0, NEG)
        if first:
            run(s, True)
        else:
            full = functools.reduce(
                jnp.logical_and, [base - CHIP * d >= sc[3 + 2 * s] for d in dists]
            )
            some = functools.reduce(
                jnp.logical_or, [base - CHIP * d + CHIP > sc[2 + 2 * s] for d in dists]
            )
            pl.when(full)(functools.partial(run, s, False))
            pl.when(some & jnp.logical_not(full))(functools.partial(run, s, True))
            if last:
                pl.when(jnp.logical_not(some))(functools.partial(finish, s))


def attend(sc, query, query_sibling, starts, pairs, dists, state=None, last=False, sides=(0, 1)):
    nk, first = len(dists), state is None
    whole = pl.BlockSpec(memory_space=VMEM)
    parts = tuple(pair[0] if isinstance(pair, tuple) else "one" for pair in pairs)
    args = [sc, query, query_sibling, starts]
    for pair in pairs:
        args += pair[1:] if isinstance(pair, tuple) else [pair]
    in_specs = [pl.BlockSpec(memory_space=pltpu.SMEM)] + [whole] * (len(args) - 1)
    aliases = {}
    if not first:
        if not last:
            aliases = {len(args) + i: i for i in range(3)}
        in_specs += [whole] * 3
        args += [pltpu.with_memory_space_constraint(x, VMEM) for x in state]
    if last:
        out_shape = [VMEM((TOK, KVH * GW * HD), jnp.bfloat16)] * len(sides)
    else:
        out_shape = [VMEM((KVH * 2 * ROWS, HD), jnp.float32)] * 3
    return pl.pallas_call(
        functools.partial(attn_kernel, tuple(dists), parts, first, last, sides),
        in_specs=in_specs,
        out_specs=[whole] * len(out_shape),
        out_shape=out_shape,
        scratch_shapes=[VMEM((2, TOK, nk * CHIP), jnp.float32), VMEM((ROWS, HD), jnp.bfloat16)],
        input_output_aliases=aliases,
        compiler_params=pltpu.CompilerParams(vmem_limit_bytes=16 << 20),
        cost_estimate=pl.CostEstimate(
            flops=KVH * len(sides) * ROWS * CHIP * nk * HD * 4, bytes_accessed=4 << 20, transcendentals=0
        ),
        name="attend_" + "_".join(str(d) for d in dists) + ("" if len(sides) == 2 else "ab"[sides[0]]),
    )(*args)


def join_kernel(sc, mine, other, out, sems):
    width = KVH * GW * HD
    copies = [
        pltpu.make_async_copy(
            part, out.at[:, pl.ds(pl.multiple_of(core * width, width), width)], sems.at[i]
        )
        for i, (part, core) in enumerate(((mine, sc[0]), (other, 1 - sc[0])))
    ]
    for copy in copies:
        copy.start()
    for copy in copies:
        copy.wait()


def join(sc, mine, other):
    whole = pl.BlockSpec(memory_space=VMEM)
    return pl.pallas_call(
        join_kernel,
        in_specs=[pl.BlockSpec(memory_space=pltpu.SMEM), whole, whole],
        out_specs=pl.BlockSpec(memory_space=pl.ANY),
        out_shape=jax.ShapeDtypeStruct((TOK, 2 * KVH * GW * HD), jnp.bfloat16),
        scratch_shapes=[pltpu.SemaphoreType.DMA((2,))],
        compiler_params=pltpu.CompilerParams(vmem_limit_bytes=16 << 20),
        name="join",
    )(sc, pltpu.with_memory_space_constraint(mine, VMEM), other)


def solution(mesh):
    outer, inner, head = (mesh.shape[axis] for axis in ("outer", "inner", "head"))
    devices = outer * inner * head

    def index_of(block):
        return (block % head) * (outer * inner) + block // head

    chips_all = devices // 2

    def send(value, moves):
        pairs = [(index_of(2 * a + k), index_of(2 * b + k)) for a, b in moves for k in range(2)]
        return lax.ppermute(value, MESH_AXES, pairs)

    def behind(value, chips, wrap=()):
        moves = [(c, (c + chips) % chips_all) for c in range(chips_all)]
        return send(value, [(c, d) for c, d in moves if d == c + chips or d in wrap])

    def swap(value):
        return lax.ppermute(
            value, MESH_AXES, [(index_of(b), index_of(b ^ 1)) for b in range(devices)]
        )

    def after(value, state):
        value, top = lax.optimization_barrier((value, state[0]))
        return value, [top, *state[1:]]

    def per_device(query, keys, values, lengths):
        block = lax.axis_index(("outer", "inner")) * head + lax.axis_index("head")
        core = lax.rem(block, 2)
        base = (block - core) * TOK
        half = KVH * HD

        def halves(first_core, second_core):
            return jnp.concatenate([first_core, second_core], axis=1)

        def heads_of(array, which, size):
            return lax.dynamic_slice_in_dim(array, which * size, size, 1)

        kv_mine = halves(heads_of(keys, core, half), heads_of(values, core, half))
        kv_send = halves(heads_of(keys, 1 - core, half), heads_of(values, 1 - core, half))
        width = KVH * GW * HD
        query_send, kv_send = lax.optimization_barrier((query, kv_send))
        query_send = heads_of(query_send, 1 - core, width)
        kv_sibling, query_send = lax.optimization_barrier((swap(kv_send), query_send))
        r0 = jnp.concatenate([kv_mine, kv_sibling], axis=0)
        query_sibling = swap(query_send)

        order = lax.iota(jnp.int32, lengths.shape[0])
        ends = jnp.sum(jnp.where(order[None, :] <= order[:, None], lengths[None, :], 0), axis=1)

        def start_of(pos):
            return jnp.max(jnp.where(ends[None, :] <= pos[:, None], ends[None, :], 0), axis=1)

        row = lax.iota(jnp.int32, CHIP)
        offset = lax.rem(row + core * TOK, CHIP)
        starts = jnp.broadcast_to(start_of(base + offset)[:, None], (CHIP, HD))
        i8 = lax.iota(jnp.int32, 8)
        pick = jnp.where(i8 == 3, TOK - 1, jnp.where(i8 == 4, TOK, jnp.where(i8 == 5, CHIP - 1, 0)))
        start8 = start_of(base + lax.rem(pick + core * TOK, CHIP))
        sc = jnp.where(
            i8 == 0, core,
            jnp.where(
                i8 == 1, base,
                jnp.where(i8 == 6, core * TOK, jnp.where(i8 == 7, (1 - core) * TOK, start8)),
            ),
        )

        call = functools.partial(attend, sc, query, query_sibling, starts)
        mid = CHIP // 2
        r4, r1 = behind(r0, 4, (0, 1)), behind(r0, 1)
        state = call([r0], (0,))
        r4, state = after(r4, state)
        r3, r8 = behind(r4, -1, (127,)), behind(r4, 4, (0,))
        r2a, r5 = behind(r1[:mid], 1), behind(r1, 4)
        state = call([r4, r1], (4, 1), state)
        r8, state = after(r8, state)
        r7 = behind(r8, -1, (127,))
        r2b = behind(r3[mid:], -1, (127,))
        r6a = behind(r2a, 4)
        state = call([r3, r8], (3, 8), state)
        r2b, state = after(r2b, state)
        r6b = behind(r2b, 4)
        state = call([("cat", r2a, r2b), r5], (2, 5), state)
        mine, sibling = call([r7, ("cat", r6a, r6b)], (7, 6), state, True)
        return join(sc, mine, swap(sibling))

    tokens = P(("outer", "inner", "head"), None)
    return jax.shard_map(
        per_device,
        mesh=mesh,
        in_specs=(tokens, tokens, tokens, P()),
        out_specs=tokens,
        check_vma=False,
    )
```

```python
import functools
import math

import jax
import jax.numpy as jnp
from jax import lax
from jax.experimental import pallas as pl
from jax.experimental.pallas import tpu as pltpu
from jax.sharding import PartitionSpec as P

HD = 128
GW = 8
KVH = 4
TOK = 128
CHIP = 256
ROWS = GW * TOK
RC = 128
SCALE = math.log2(math.e) / math.sqrt(HD)
NEG = -1e30
MESH_AXES = ("head", "outer", "inner")
VMEM = pltpu.VMEM


def attn_kernel(dists, parts, first, last, sides, *refs):
    nk = len(dists)
    sc, query, query_sibling, st = refs[:4]
    pos = 4
    pairs = []
    for part in parts:
        count = 1 if part == "one" else 2
        pairs.append((part, refs[pos : pos + count]))
        pos += count
    if not first:
        m_in, l_in, a_in = refs[pos : pos + 3]
        pos += 3
    if last:
        outs = dict(zip(sides, refs[pos : pos + len(sides)]))
        pos += len(sides)
    else:
        m_out, l_out, a_out = refs[pos : pos + 3]
        pos += 3
    bias, qs = refs[pos : pos + 2]
    base = sc[1]

    def lanes(start, offset=0):
        return pl.ds(pl.multiple_of(start, HD) + offset, HD)

    def columns(pair, at):
        part, arrays = pair
        loaded = [array[:, at] for array in arrays]
        if part == "cat":
            return jnp.concatenate(loaded, axis=0)
        return loaded[0] + loaded[1] if part == "add" else loaded[0]

    def run(s, masked):
        @pl.loop(0, KVH)
        def _(g):
            source = (query, query_sibling)[s]
            shift = sc[0] * (KVH * GW * HD) if s == 0 else 0
            for h in range(GW):
                qs[h * TOK : (h + 1) * TOK, :] = source[:, lanes(shift + g * (GW * HD) + h * HD)]
            ones = jnp.ones((CHIP, HD), jnp.bfloat16)
            ks = [columns(p, lanes(g * HD)) for p in pairs]
            vs = [
                jnp.concatenate([columns(p, lanes((KVH + g) * HD)), ones], axis=1) for p in pairs
            ]
            for r0 in range(0, ROWS, RC):
                scores = []
                for j in range(nk):
                    x = lax.dot_general(
                        qs[r0 : r0 + RC, :], ks[j], (((1,), (1,)), ((), ())),
                        preferred_element_type=jnp.float32,
                    )
                    if masked:
                        b = bias[s, :, j * CHIP : (j + 1) * CHIP]
                        x = (x.reshape(RC // TOK, TOK, CHIP) + b[None]).reshape(RC, CHIP)
                    scores.append(x)
                top = jnp.max(functools.reduce(jnp.maximum, scores), axis=1, keepdims=True)
                top = jnp.broadcast_to(top * SCALE, (RC, HD))
                rows = pl.ds(pl.multiple_of((g * 2 + s) * ROWS, ROWS) + r0, RC)
                if not first:
                    before = m_in[rows, :]
                    top = jnp.maximum(before, top)
                    shrink = jnp.exp2(before - top)
                tops = jnp.concatenate([top, top], axis=1)
                both = None
                for j in range(nk):
                    p = jnp.exp2(scores[j] * SCALE - tops).astype(jnp.bfloat16)
                    d = lax.dot_general(
                        p, vs[j], (((1,), (0,)), ((), ())), preferred_element_type=jnp.float32
                    )
                    both = d if both is None else both + d
                a, l = both[:, :HD], both[:, HD:]
                if not first:
                    a = a + a_in[rows, :] * shrink
                    l = l + l_in[rows, :] * shrink
                if last:
                    o = (a / l).astype(jnp.bfloat16)
                    for i in range(RC // TOK):
                        outs[s][:, lanes(g * (GW * HD), r0 // TOK * HD + i * HD)] = o[
                            i * TOK : (i + 1) * TOK, :
                        ]
                else:
                    m_out[rows, :] = top
                    l_out[rows, :] = l
                    a_out[rows, :] = a

    def finish(s):
        @pl.loop(0, KVH)
        def _(g):
            for h in range(GW):
                rows = pl.ds(pl.multiple_of((g * 2 + s) * ROWS, ROWS) + h * TOK, TOK)
                outs[s][:, lanes(g * (GW * HD), h * HD)] = (a_in[rows, :] / l_in[rows, :]).astype(
                    jnp.bfloat16
                )

    for s in sides:
        starts = st[s * TOK : (s + 1) * TOK, :1]
        query_pos = base + sc[6 + s] + lax.broadcasted_iota(jnp.int32, (TOK, CHIP), 0)
        for j, d in enumerate(dists):
            key = lax.broadcasted_iota(jnp.int32, (TOK, CHIP), 1)
            key_pos = base - CHIP * d + ((key + sc[6]) & (CHIP - 1))
            visible = key_pos >= starts
            if d == 0:
                visible = visible & (key_pos <= query_pos)
            bias[s, :, j * CHIP : (j + 1) * CHIP] = jnp.where(visible, 0.0, NEG)
        if first:
            run(s, True)
        else:
            full = functools.reduce(
                jnp.logical_and, [base - CHIP * d >= sc[3 + 2 * s] for d in dists]
            )
            some = functools.reduce(
                jnp.logical_or, [base - CHIP * d + CHIP > sc[2 + 2 * s] for d in dists]
            )
            pl.when(full)(functools.partial(run, s, False))
            pl.when(some & jnp.logical_not(full))(functools.partial(run, s, True))
            if last:
                pl.when(jnp.logical_not(some))(functools.partial(finish, s))


def attend(sc, query, query_sibling, starts, pairs, dists, state=None, last=False, sides=(0, 1)):
    nk, first = len(dists), state is None
    whole = pl.BlockSpec(memory_space=VMEM)
    parts = tuple(pair[0] if isinstance(pair, tuple) else "one" for pair in pairs)
    args = [sc, query, query_sibling, starts]
    for pair in pairs:
        args += pair[1:] if isinstance(pair, tuple) else [pair]
    in_specs = [pl.BlockSpec(memory_space=pltpu.SMEM)] + [whole] * (len(args) - 1)
    aliases = {}
    if not first:
        if not last:
            aliases = {len(args) + i: i for i in range(3)}
        in_specs += [whole] * 3
        args += [pltpu.with_memory_space_constraint(x, VMEM) for x in state]
    if last:
        out_shape = [VMEM((TOK, KVH * GW * HD), jnp.bfloat16)] * len(sides)
    else:
        out_shape = [VMEM((KVH * 2 * ROWS, HD), jnp.float32)] * 3
    return pl.pallas_call(
        functools.partial(attn_kernel, tuple(dists), parts, first, last, sides),
        in_specs=in_specs,
        out_specs=[whole] * len(out_shape),
        out_shape=out_shape,
        scratch_shapes=[VMEM((2, TOK, nk * CHIP), jnp.float32), VMEM((ROWS, HD), jnp.bfloat16)],
        input_output_aliases=aliases,
        compiler_params=pltpu.CompilerParams(vmem_limit_bytes=16 << 20),
        cost_estimate=pl.CostEstimate(
            flops=KVH * len(sides) * ROWS * CHIP * nk * HD * 4, bytes_accessed=4 << 20, transcendentals=0
        ),
        name="attend_" + "_".join(str(d) for d in dists) + ("" if len(sides) == 2 else "ab"[sides[0]]),
    )(*args)


def join_kernel(sc, mine, other, out, sems):
    width = KVH * GW * HD
    copies = [
        pltpu.make_async_copy(
            part, out.at[:, pl.ds(pl.multiple_of(core * width, width), width)], sems.at[i]
        )
        for i, (part, core) in enumerate(((mine, sc[0]), (other, 1 - sc[0])))
    ]
    for copy in copies:
        copy.start()
    for copy in copies:
        copy.wait()


def join(sc, mine, other):
    whole = pl.BlockSpec(memory_space=VMEM)
    return pl.pallas_call(
        join_kernel,
        in_specs=[pl.BlockSpec(memory_space=pltpu.SMEM), whole, whole],
        out_specs=pl.BlockSpec(memory_space=pl.ANY),
        out_shape=jax.ShapeDtypeStruct((TOK, 2 * KVH * GW * HD), jnp.bfloat16),
        scratch_shapes=[pltpu.SemaphoreType.DMA((2,))],
        compiler_params=pltpu.CompilerParams(vmem_limit_bytes=16 << 20),
        name="join",
    )(sc, pltpu.with_memory_space_constraint(mine, VMEM), other)


def solution(mesh):
    outer, inner, head = (mesh.shape[axis] for axis in ("outer", "inner", "head"))
    devices = outer * inner * head

    def index_of(block):
        return (block % head) * (outer * inner) + block // head

    chips_all = devices // 2

    def send(value, moves):
        pairs = [(index_of(2 * a + k), index_of(2 * b + k)) for a, b in moves for k in range(2)]
        return lax.ppermute(value, MESH_AXES, pairs)

    def behind(value, chips, wrap=()):
        moves = [(c, (c + chips) % chips_all) for c in range(chips_all)]
        return send(value, [(c, d) for c, d in moves if d == c + chips or d in wrap])

    def swap(value):
        return lax.ppermute(
            value, MESH_AXES, [(index_of(b), index_of(b ^ 1)) for b in range(devices)]
        )

    def after(value, state):
        value, top = lax.optimization_barrier((value, state[0]))
        return value, [top, *state[1:]]

    def per_device(query, keys, values, lengths):
        block = lax.axis_index(("outer", "inner")) * head + lax.axis_index("head")
        core = lax.rem(block, 2)
        base = (block - core) * TOK
        half = KVH * HD

        def halves(first_core, second_core):
            return jnp.concatenate([first_core, second_core], axis=1)

        def heads_of(array, which, size):
            return lax.dynamic_slice_in_dim(array, which * size, size, 1)

        kv_mine = halves(heads_of(keys, core, half), heads_of(values, core, half))
        kv_send = halves(heads_of(keys, 1 - core, half), heads_of(values, 1 - core, half))
        width = KVH * GW * HD
        query_send, kv_send = lax.optimization_barrier((query, kv_send))
        query_send = heads_of(query_send, 1 - core, width)
        kv_sibling, query_send = lax.optimization_barrier((swap(kv_send), query_send))
        r0 = jnp.concatenate([kv_mine, kv_sibling], axis=0)
        query_sibling = swap(query_send)

        order = lax.iota(jnp.int32, lengths.shape[0])
        ends = jnp.sum(jnp.where(order[None, :] <= order[:, None], lengths[None, :], 0), axis=1)

        def start_of(pos):
            return jnp.max(jnp.where(ends[None, :] <= pos[:, None], ends[None, :], 0), axis=1)

        row = lax.iota(jnp.int32, CHIP)
        offset = lax.rem(row + core * TOK, CHIP)
        starts = jnp.broadcast_to(start_of(base + offset)[:, None], (CHIP, HD))
        i8 = lax.iota(jnp.int32, 8)
        pick = jnp.where(i8 == 3, TOK - 1, jnp.where(i8 == 4, TOK, jnp.where(i8 == 5, CHIP - 1, 0)))
        start8 = start_of(base + lax.rem(pick + core * TOK, CHIP))
        sc = jnp.where(
            i8 == 0, core,
            jnp.where(
                i8 == 1, base,
                jnp.where(i8 == 6, core * TOK, jnp.where(i8 == 7, (1 - core) * TOK, start8)),
            ),
        )

        call = functools.partial(attend, sc, query, query_sibling, starts)
        mid = CHIP // 2
        r4, r1 = behind(r0, 4, (0, 1)), behind(r0, 1)
        state = call([r0], (0,))
        r4, state = after(r4, state)
        r3, r8 = behind(r4, -1, (127,)), behind(r4, 4, (0,))
        r2a = behind(r1[:mid], 1)
        state = call([r4, r1], (4, 1), state)
        r1, state = after(r1, state)
        r5 = behind(r1, 4)
        r8, state = after(r8, state)
        r7 = behind(r8, -1, (127,))
        r2b = behind(r3[mid:], -1, (127,))
        state = call([r3, r8], (3, 8), state)
        r2a, state = after(r2a, state)
        r2b, state = after(r2b, state)
        r6a, r6b = behind(r2a, 4), behind(r2b, 4)
        state = call([("cat", r2a, r2b), r5], (2, 5), state)
        mine, sibling = call([r7, ("cat", r6a, r6b)], (7, 6), state, True)
        return join(sc, mine, swap(sibling))

    tokens = P(("outer", "inner", "head"), None)
    return jax.shard_map(
        per_device,
        mesh=mesh,
        in_specs=(tokens, tokens, tokens, P()),
        out_specs=tokens,
        check_vma=False,
    )
```
